256 devices in a mesh: dev: 128 (over y, x, z), rep: 2 (over core).
Axes of the slice: x: 4, y: 4, z: 8, core: 2. Of those that a mesh axis runs over, the one named last changes fastest.
Arguments:
- embeddings: float32 [32768, 4096], P(('rep', 'dev')), parts along dimension 0, may hold values from -130 to 130
- cluster_id: int32 [32768], P(('rep', 'dev')), parts along dimension 0, may hold values from 0 to 255, as said below
- member_order: int32 [32768], P(('rep', 'dev')), parts along dimension 0, may hold values from 0 to 127, as said below
- cluster_slot: int32 [512], P('rep'), parts along dimension 0, may hold values from 0 to 255, each once
- cluster_size: int32 [512], P('rep'), parts along dimension 0, may hold values from 16 to 128, as said below
Outputs:
- best_similarity: float32 [32768], P(('rep', 'dev')), parts along dimension 0
- keep: int32 [32768], P(('rep', 'dev')), parts along dimension 0
- cluster_mean: float32 [512], P(('rep', 'dev')), parts along dimension 0
The draws below stay inside these ranges and needn't reach their ends.
There are 2 independent parts, one for each index of `rep`. The reference program is written for one: setup_inputs(seed, part) draws one part's arguments, and reference() takes and returns one part's arrays. A program takes and returns all parts, laid end to end along the dimension named above; each array names one. Nothing has to cross between parts.
Inputs may be any that keep to these rules, and one draw needn't show every extreme that they name: `cluster_id`: every cluster holds at most 128 rows and some cluster exactly 128. A cluster of n members has floor(n / 128) or ceil(n / 128) of them among the rows of each device, so at most 1, a number reached on every device. `member_order`: within a cluster of n members the ranks are 0 to n - 1, each once. `cluster_slot`: a permutation; cluster c is owned by device cluster_slot[c] // 2 of dev. `cluster_size`: the number of rows whose cluster_id is c.
All inputs are finite; a program needn't handle non-finite values.
Results may differ from the reference program's by a relative error of at most 0.0003.
Values may be sent and summed in bfloat16 or wider, within the bound.
A program may use at most 64 MiB of HBM per device.

```python
import jax
import jax.numpy as jnp
from jax import lax

D = 4096
CAP = 128
CLUSTERS = 256
ROWS_ALL = 16384
N_DEV = 128


def layout(key):
    base_key = jax.random.fold_in(key, 7)
    key_sizes, key_labels, key_order, key_source, key_rows = jax.random.split(base_key, 5)
    half_count = CLUSTERS // 2
    sizes_pair = jax.random.randint(key_sizes, (half_count,), CAP // 8, CAP - CAP // 8 + 1)
    base_sizes = jnp.concatenate([sizes_pair, CAP - sizes_pair]).astype(jnp.int32)
    base_sizes = base_sizes.at[0].set(CAP).at[half_count].set(CAP // 2).at[1].set(CAP // 4).at[half_count + 1].set(CAP // 4)
    labels = jax.random.permutation(key_labels, CLUSTERS)
    sizes_out = jnp.zeros((CLUSTERS,), jnp.int32).at[labels].set(base_sizes)
    size_ends = jnp.cumsum(sizes_out)
    size_starts = size_ends - sizes_out
    positions = jnp.arange(ROWS_ALL, dtype=jnp.int32)
    owner_cluster = jnp.sum((positions[:, None] >= size_ends[None, :]).astype(jnp.int32), axis=1)
    shuffle = jax.random.permutation(key_order, ROWS_ALL).astype(jnp.int32)
    ranked = jnp.argsort(owner_cluster * ROWS_ALL + shuffle, stable=True)
    inverse = jnp.zeros((ROWS_ALL,), jnp.int32).at[ranked].set(positions)
    orders = inverse - size_starts[owner_cluster]
    source_perm = jax.random.permutation(key_source, N_DEV).astype(jnp.int32)
    source = source_perm[positions % N_DEV]
    second = jax.random.permutation(key_rows, ROWS_ALL).astype(jnp.int32)
    placed = jnp.argsort(source * ROWS_ALL + second, stable=True)
    target = jnp.zeros((ROWS_ALL,), jnp.int32).at[placed].set(positions)
    ids_out = jnp.zeros((ROWS_ALL,), jnp.int32).at[target].set(owner_cluster)
    order_out = jnp.zeros((ROWS_ALL,), jnp.int32).at[target].set(orders)
    return (ids_out, order_out, sizes_out)


def draw_cluster_id(key, part):
    return layout(key)[0]


def draw_member_order(key, part):
    return layout(key)[1]


def draw_cluster_size(key, part):
    return layout(key)[2]


def draw_embeddings(key, part):
    cluster_ids = layout(key)[0]
    base_key = jax.random.fold_in(key, 11)
    key_anchor, key_noise, key_copy = jax.random.split(base_key, 3)
    anchors = jnp.clip(jax.random.normal(key_anchor, (CLUSTERS, D), jnp.float32), -8.0, 8.0)
    noise = jnp.clip(jax.random.normal(key_noise, (ROWS_ALL, D), jnp.float32), -8.0, 8.0)
    copied = jax.random.randint(key_copy, (ROWS_ALL,), 0, 3) == 0
    values = jnp.where(copied[:, None], anchors[cluster_ids] + 0.15 * noise, noise)
    return values.astype(jnp.float32)


def setup_inputs(seed: int = 0, part: int = 0) -> dict:
    key_list = jax.random.split(jax.random.key(seed), 6)
    own_keys = jax.random.split(jax.random.fold_in(key_list[5], part), 6)
    embeddings = draw_embeddings(jax.random.fold_in(jax.random.fold_in(key_list[5], part), 71), part)
    cluster_id = draw_cluster_id(jax.random.fold_in(jax.random.fold_in(key_list[5], part), 71), part)
    member_order = draw_member_order(jax.random.fold_in(jax.random.fold_in(key_list[5], part), 71), part)
    cluster_slot = jax.random.permutation(own_keys[3], CLUSTERS).astype(jnp.int32)
    cluster_size = draw_cluster_size(jax.random.fold_in(jax.random.fold_in(key_list[5], part), 71), part)
    return {"embeddings": embeddings, "cluster_id": cluster_id, "member_order": member_order, "cluster_slot": cluster_slot, "cluster_size": cluster_size}


norm_eps = 1e-06
cutoff = 0.8

def normalized(values):
    squares_sum = lax.optimization_barrier(jnp.sum(values * values, axis=1, keepdims=True))
    return (values * lax.rsqrt(squares_sum + norm_eps)).astype(jnp.bfloat16)

def reference(embeddings, cluster_id, member_order, cluster_slot, cluster_size):
    unit_rows = normalized(embeddings)
    total_rows = embeddings.shape[0]
    where_put = (cluster_id * CAP + member_order).astype(jnp.int32)
    index_table = jnp.zeros((CLUSTERS * CAP,), jnp.int32).at[where_put].set(jnp.arange(total_rows, dtype=jnp.int32) + 1).reshape(CLUSTERS, CAP)
    spot_index = jnp.arange(CAP, dtype=jnp.int32)
    lower = spot_index[None, :] < spot_index[:, None]

    def one_cluster(packed):
        entries, size_now = packed
        occupied = entries > 0
        gathered = unit_rows[jnp.maximum(entries - 1, 0)].astype(jnp.float32)
        members = jnp.where(occupied[:, None], gathered, 0.0)
        is_live = occupied & (spot_index < size_now)
        similar = jnp.dot(members, members.T, preferred_element_type=jnp.float32)
        allowed = lower & is_live[None, :]
        nearest = lax.optimization_barrier(jnp.max(jnp.where(allowed, similar, -1.0), axis=1))
        best_spot = jnp.where(is_live, nearest, -1.0)
        mean_best = jnp.sum(jnp.where(is_live, best_spot, 0.0)) / size_now.astype(jnp.float32)
        return (best_spot, mean_best)
    best_table, cluster_means = lax.map(one_cluster, (index_table, cluster_size))
    row_best = best_table.reshape(-1)[where_put]
    keep_mask = (row_best < cutoff).astype(jnp.int32)
    by_slot = jnp.zeros((CLUSTERS,), jnp.float32).at[cluster_slot].set(cluster_means)
    return (row_best, keep_mask, by_slot)
```

```python
import functools

import jax
import jax.numpy as jnp
from jax import lax
from jax.experimental import pallas as pl
from jax.experimental.pallas import tpu as pltpu
from jax.sharding import PartitionSpec as P

norm_eps = 1e-06
cutoff = 0.8
MESH = pl.DeviceIdType.MESH
NY, NX, NZ = 4, 4, 8
N = NY * NX * NZ
OFFSETS = [(i // (NX * NZ), i // NZ % NX, i % NZ) for i in range(N)]
TAG = 128


def shifted(me, dy, dx, dz):
    y, x, z = me // (NX * NZ), me // NZ % NX, me % NZ
    return (y + dy) % NY * (NX * NZ) + (x + dx) % NX * NZ + (z + dz) % NZ


def peer(me, i):
    return shifted(me, *OFFSETS[i])


def source(me, i):
    dy, dx, dz = OFFSETS[i]
    return shifted(me, NY - dy, NX - dx, NZ - dz)


def hops(i):
    return sum(min(d, n - d) for d, n in zip(OFFSETS[i], (NY, NX, NZ)))


FAR_FIRST = sorted(range(1, N), key=lambda i: -hops(i))
SEMS = N // NZ + NZ


def flag(i):
    return i // NZ if i >= NZ else N // NZ + i


def exchange(src, dst, send_sem, recv_sem, target):
    for i in FAR_FIRST:
        pair = pl.ds(2 * i, 2)
        pltpu.make_async_remote_copy(
            src.at[pair], dst.at[pair], send_sem.at[flag(i)], recv_sem.at[flag(i)],
            device_id={"dev": target(i)}, device_id_type=MESH,
        ).start()


def waits(src, dst, send_sem, recv_sem, target):
    for g in range(1, N // NZ):
        part = pl.ds(2 * NZ * g, 2 * NZ)
        yield pltpu.make_async_remote_copy(
            src.at[part], dst.at[part], send_sem.at[g], recv_sem.at[g],
            device_id={"dev": target(1)}, device_id_type=MESH,
        )
    for i in range(1, NZ):
        pair = pl.ds(2 * i, 2)
        yield pltpu.make_async_remote_copy(
            src.at[pair], dst.at[pair], send_sem.at[flag(i)], recv_sem.at[flag(i)],
            device_id={"dev": target(1)}, device_id_type=MESH,
        )


def kernel(emb_ref, id_hbm, order_hbm, slot_hbm, size_hbm, best_ref, keep_ref, mean_ref,
           id_ref, order_ref, slot_ref, size_ref, raw, unit, packed, got, answers, returned, load_sem, own_sem, send_sem, recv_sem, back_send, back_recv):
    me = lax.axis_index("dev")
    rows, width = raw.shape
    slots = packed.shape[0]
    pieces = 4
    step = rows // pieces
    smalls = []
    for p, (src, dst) in enumerate(
        ((id_hbm, id_ref), (slot_hbm, slot_ref), (order_hbm, order_ref), (size_hbm, size_ref))
    ):
        load = pltpu.make_async_copy(src, dst, load_sem.at[pieces + p])
        load.start()
        smalls.append(load)
    loads = []
    for p in range(pieces):
        part = pl.ds(p * step, step)
        load = pltpu.make_async_copy(emb_ref.at[part], raw.at[part], load_sem.at[p])
        load.start()
        loads.append(load)
    barrier = pltpu.get_barrier_semaphore()
    for i in FAR_FIRST:
        pl.semaphore_signal(barrier, inc=1, device_id={"dev": peer(me, i)}, device_id_type=MESH)

    for load in smalls:
        load.wait()
    member = lax.broadcasted_iota(jnp.int32, (slots, rows), 0) == id_ref[...]
    table = jnp.broadcast_to(slot_ref[...].astype(jnp.bfloat16), (8, slots))
    slot_row = jnp.dot(table, member.astype(jnp.bfloat16), preferred_element_type=jnp.float32)[0:1]
    slot_row = slot_row.astype(jnp.int32)
    place = lax.broadcasted_iota(jnp.int32, (slots, rows), 0)
    offset = place // 2
    goal = shifted(me, offset // (NX * NZ), offset // NZ % NX, offset % NZ)
    chosen = slot_row == goal * 2 + place % 2
    pick = chosen.astype(jnp.bfloat16)
    rank_next = (order_ref[...] + 1).astype(jnp.float32)
    tag = jnp.sum(jnp.where(chosen, rank_next, 0.0), axis=1, keepdims=True)
    packed[:, width:] = jnp.broadcast_to(tag, (slots, TAG)).astype(jnp.bfloat16)

    for p in range(pieces):
        loads[p].wait()
        part = pl.ds(p * step, step)
        values = raw[part]
        squares_sum = jnp.sum(values * values, axis=1, keepdims=True)
        unit[part] = (values * lax.rsqrt(squares_sum + norm_eps)).astype(jnp.bfloat16)
    chunk = 512
    for k in range(0, width, chunk):
        packed[:, k:k + chunk] = jnp.dot(
            pick, unit[:, k:k + chunk], preferred_element_type=jnp.float32
        ).astype(jnp.bfloat16)

    pl.semaphore_wait(barrier, N - 1)
    there = (packed, got, send_sem, recv_sem, functools.partial(peer, me))
    exchange(*there)
    own = pltpu.make_async_copy(packed.at[pl.ds(0, 2)], got.at[pl.ds(0, 2)], own_sem)
    own.start()
    own.wait()
    for copy in waits(*there):
        copy.wait_recv()

    similar = jnp.zeros((slots, slots), jnp.float32)
    chunk = 1024
    for k in range(0, width, chunk):
        block = got[:, k:k + chunk]
        similar += lax.dot_general(block, block, (((1,), (1,)), ((), ())), preferred_element_type=jnp.float32)
    tags = got[:, width:]
    first = (lax.broadcasted_iota(jnp.int32, (8, TAG), 1) == 0).astype(jnp.bfloat16)
    rank_j = lax.dot_general(first, tags, (((1,), (1,)), ((), ())), preferred_element_type=jnp.float32)[0:1]
    rank_i = tags[:, 0:1].astype(jnp.float32)
    sizes = [
        jnp.sum(jnp.where(slot_ref[...] == 2 * me + b, size_ref[...], 0), axis=1, keepdims=True).astype(jnp.float32)
        for b in range(2)
    ]
    side_i = lax.broadcasted_iota(jnp.int32, (slots, 1), 0) % 2
    side_j = lax.broadcasted_iota(jnp.int32, (1, slots), 1) % 2
    live_i = (rank_i > 0.0) & (rank_i <= jnp.where(side_i == 0, sizes[0], sizes[1]))
    live_j = (rank_j > 0.0) & (rank_j <= jnp.where(side_j == 0, sizes[0], sizes[1]))
    mark_j = jnp.where(live_j, rank_j, 1024.0)
    allowed = (side_i == side_j) & (mark_j < rank_i)
    nearest = jnp.max(jnp.where(allowed, similar, -1.0), axis=1, keepdims=True)
    best = jnp.where(live_i, nearest, -1.0)
    answers[...] = jnp.broadcast_to(best, answers.shape)

    back = (answers, returned, back_send, back_recv, functools.partial(source, me))
    exchange(*back)
    own = pltpu.make_async_copy(answers.at[pl.ds(0, 2)], returned.at[pl.ds(0, 2)], own_sem)
    own.start()
    lane = lax.broadcasted_iota(jnp.int32, (1, 128), 1)
    means = [
        jnp.sum(jnp.where(live_i & (side_i == b), best, 0.0), axis=0, keepdims=True) / sizes[b]
        for b in range(2)
    ]
    mean_ref[...] = jnp.where(lane == 0, means[0], means[1])
    own.wait()
    for copy in waits(*back):
        copy.wait_recv()
    row_best = jnp.max(jnp.where(chosen, returned[...], -2.0), axis=0, keepdims=True)
    best_ref[...] = row_best
    keep_ref[...] = (row_best < cutoff).astype(jnp.int32)
    for copy in (*waits(*there), *waits(*back)):
        copy.wait_send()


def body(embeddings, cluster_id, member_order, cluster_slot, cluster_size):
    rows, width = embeddings.shape
    clusters = cluster_slot.shape[0]
    slots = clusters
    vmem = pl.BlockSpec(memory_space=pltpu.VMEM)
    best, keep, mean = pl.pallas_call(
        kernel,
        out_shape=(
            jax.ShapeDtypeStruct((1, rows), jnp.float32),
            jax.ShapeDtypeStruct((1, rows), jnp.int32),
            jax.ShapeDtypeStruct((1, 128), jnp.float32),
        ),
        in_specs=[pl.BlockSpec(memory_space=pltpu.HBM)] * 5,
        out_specs=(vmem, vmem, vmem),
        scratch_shapes=[
            pltpu.VMEM((1, rows), jnp.int32),
            pltpu.VMEM((1, rows), jnp.int32),
            pltpu.VMEM((1, clusters), jnp.int32),
            pltpu.VMEM((1, clusters), jnp.int32),
            pltpu.VMEM((rows, width), jnp.float32),
            pltpu.VMEM((rows, width), jnp.bfloat16),
            pltpu.VMEM((slots, width + TAG), jnp.bfloat16),
            pltpu.VMEM((slots, width + TAG), jnp.bfloat16),
            pltpu.VMEM((slots, 128), jnp.float32),
            pltpu.VMEM((slots, 128), jnp.float32),
            pltpu.SemaphoreType.DMA((8,)),
            pltpu.SemaphoreType.DMA,
            pltpu.SemaphoreType.DMA((SEMS,)),
            pltpu.SemaphoreType.DMA((SEMS,)),
            pltpu.SemaphoreType.DMA((SEMS,)),
            pltpu.SemaphoreType.DMA((SEMS,)),
        ],
        compiler_params=pltpu.CompilerParams(collective_id=0, has_side_effects=True, vmem_limit_bytes=67_043_328),
    )(embeddings, cluster_id[None], member_order[None], cluster_slot[None], cluster_size[None])
    return best[0], keep[0], mean[0, : clusters // N]


def solution(mesh):
    placed = (P(("rep", "dev"), None), P(("rep", "dev")), P(("rep", "dev")), P("rep"), P("rep"))
    return jax.shard_map(
        body,
        mesh=mesh,
        in_specs=placed,
        out_specs=(P(("rep", "dev")), P(("rep", "dev")), P(("rep", "dev"))),
        check_vma=False,
    )
```

```python
import functools

import jax
import jax.numpy as jnp
from jax import lax
from jax.experimental import pallas as pl
from jax.experimental.pallas import tpu as pltpu
from jax.sharding import PartitionSpec as P

norm_eps = 1e-06
cutoff = 0.8
MESH = pl.DeviceIdType.MESH
NY, NX, NZ = 4, 4, 8
N = NY * NX * NZ
OFFSETS = [(i // (NX * NZ), i // NZ % NX, i % NZ) for i in range(N)]
TAG = 128


def shifted(me, dy, dx, dz):
    y, x, z = me // (NX * NZ), me // NZ % NX, me % NZ
    return (y + dy) % NY * (NX * NZ) + (x + dx) % NX * NZ + (z + dz) % NZ


def peer(me, i):
    return shifted(me, *OFFSETS[i])


def source(me, i):
    dy, dx, dz = OFFSETS[i]
    return shifted(me, NY - dy, NX - dx, NZ - dz)


def hops(i):
    return sum(min(d, n - d) for d, n in zip(OFFSETS[i], (NY, NX, NZ)))


FAR_FIRST = sorted(range(1, N), key=lambda i: -hops(i))
SEMS = N // NZ + NZ


def flag(i):
    return i // NZ if i >= NZ else N // NZ + i


def exchange(src, dst, send_sem, recv_sem, target, unit):
    for i in FAR_FIRST:
        pair = pl.ds(unit * i, unit)
        pltpu.make_async_remote_copy(
            src.at[pair], dst.at[pair], send_sem.at[flag(i)], recv_sem.at[flag(i)],
            device_id={"dev": target(i)}, device_id_type=MESH,
        ).start()


def waits(src, dst, send_sem, recv_sem, target, unit):
    for g in range(1, N // NZ):
        part = pl.ds(unit * NZ * g, unit * NZ)
        yield pltpu.make_async_remote_copy(
            src.at[part], dst.at[part], send_sem.at[g], recv_sem.at[g],
            device_id={"dev": target(1)}, device_id_type=MESH,
        )
    for i in range(1, NZ):
        pair = pl.ds(unit * i, unit)
        yield pltpu.make_async_remote_copy(
            src.at[pair], dst.at[pair], send_sem.at[flag(i)], recv_sem.at[flag(i)],
            device_id={"dev": target(1)}, device_id_type=MESH,
        )


def kernel(emb_ref, id_hbm, order_hbm, slot_hbm, size_hbm, best_ref, mean_ref,
           id_ref, order_ref, slot_ref, size_ref, raw, unit, packed, got, spread, answers, returned, load_sem, own_sem, send_sem, recv_sem, back_send, back_recv):
    me = lax.axis_index("dev")
    rows, width = raw.shape
    slots = packed.shape[0]
    pieces = 4
    step = rows // pieces
    smalls = []
    for p, (src, dst) in enumerate(
        ((id_hbm, id_ref), (slot_hbm, slot_ref), (order_hbm, order_ref), (size_hbm, size_ref))
    ):
        load = pltpu.make_async_copy(src, dst, load_sem.at[pieces + p])
        load.start()
        smalls.append(load)
    loads = []
    for p in range(pieces):
        part = pl.ds(p * step, step)
        load = pltpu.make_async_copy(emb_ref.at[part], raw.at[part], load_sem.at[p])
        load.start()
        loads.append(load)
    barrier = pltpu.get_barrier_semaphore()
    for i in FAR_FIRST:
        pl.semaphore_signal(barrier, inc=1, device_id={"dev": peer(me, i)}, device_id_type=MESH)

    for load in smalls:
        load.wait()
    member = lax.broadcasted_iota(jnp.int32, (slots, rows), 0) == id_ref[...]
    table = jnp.broadcast_to(slot_ref[...].astype(jnp.bfloat16), (8, slots))
    slot_row = jnp.dot(table, member.astype(jnp.bfloat16), preferred_element_type=jnp.float32)[0:1]
    slot_row = slot_row.astype(jnp.int32)
    place = lax.broadcasted_iota(jnp.int32, (slots, rows), 0)
    offset = place // 2
    goal = shifted(me, offset // (NX * NZ), offset // NZ % NX, offset % NZ)
    chosen = slot_row == goal * 2 + place % 2
    pick = chosen.astype(jnp.bfloat16)
    rank_next = (order_ref[...] + 1).astype(jnp.float32)
    tag = jnp.sum(jnp.where(chosen, rank_next, 0.0), axis=1, keepdims=True)
    packed[:, width:] = jnp.broadcast_to(tag, (slots, TAG)).astype(jnp.bfloat16)

    for p in range(pieces):
        loads[p].wait()
        part = pl.ds(p * step, step)
        values = raw[part]
        squares_sum = jnp.sum(values * values, axis=1, keepdims=True)
        unit[part] = (values * lax.rsqrt(squares_sum + norm_eps)).astype(jnp.bfloat16)
    chunk = 512
    for k in range(0, width, chunk):
        packed[:, k:k + chunk] = jnp.dot(
            pick, unit[:, k:k + chunk], preferred_element_type=jnp.float32
        ).astype(jnp.bfloat16)

    pl.semaphore_wait(barrier, N - 1)
    there = (packed, got, send_sem, recv_sem, functools.partial(peer, me), 2)
    exchange(*there)
    own = pltpu.make_async_copy(packed.at[pl.ds(0, 2)], got.at[pl.ds(0, 2)], own_sem)
    own.start()
    own.wait()
    for copy in waits(*there):
        copy.wait_recv()

    similar = jnp.zeros((slots, slots), jnp.float32)
    chunk = 1024
    for k in range(0, width, chunk):
        block = got[:, k:k + chunk]
        similar += lax.dot_general(block, block, (((1,), (1,)), ((), ())), preferred_element_type=jnp.float32)
    tags = got[:, width:]
    first = (lax.broadcasted_iota(jnp.int32, (8, TAG), 1) == 0).astype(jnp.bfloat16)
    rank_j = lax.dot_general(first, tags, (((1,), (1,)), ((), ())), preferred_element_type=jnp.float32)[0:1]
    rank_i = tags[:, 0:1].astype(jnp.float32)
    sizes = [
        jnp.sum(jnp.where(slot_ref[...] == 2 * me + b, size_ref[...], 0), axis=1, keepdims=True).astype(jnp.float32)
        for b in range(2)
    ]
    side_i = lax.broadcasted_iota(jnp.int32, (slots, 1), 0) % 2
    side_j = lax.broadcasted_iota(jnp.int32, (1, slots), 1) % 2
    live_i = (rank_i > 0.0) & (rank_i <= jnp.where(side_i == 0, sizes[0], sizes[1]))
    live_j = (rank_j > 0.0) & (rank_j <= jnp.where(side_j == 0, sizes[0], sizes[1]))
    mark_j = jnp.where(live_j, rank_j, 1024.0)
    allowed = (side_i == side_j) & (mark_j < rank_i)
    nearest = jnp.max(jnp.where(allowed, similar, -1.0), axis=1, keepdims=True)
    best = jnp.where(live_i, nearest, -1.0)
    spread[...] = jnp.broadcast_to(best, spread.shape)
    halves = [spread[pl.ds(b, N, stride=2), :] for b in range(2)]
    lane = lax.broadcasted_iota(jnp.int32, (1, 128), 1)
    answers[...] = jnp.where(lane < 64, halves[0], halves[1])

    back = (answers, returned, back_send, back_recv, functools.partial(source, me), 1)
    exchange(*back)
    own = pltpu.make_async_copy(answers.at[pl.ds(0, 1)], returned.at[pl.ds(0, 1)], own_sem)
    own.start()
    means = [
        jnp.sum(jnp.where(live_i & (side_i == b), best, 0.0), axis=0, keepdims=True) / sizes[b]
        for b in range(2)
    ]
    mean_ref[...] = jnp.where(lane == 0, means[0], means[1])
    own.wait()
    for copy in waits(*back):
        copy.wait_recv()
    offset = lax.broadcasted_iota(jnp.int32, (N, rows), 0)
    goal = shifted(me, offset // (NX * NZ), offset // NZ % NX, offset % NZ)
    row_best = jnp.full((1, rows), -2.0, jnp.float32)
    for b in range(2):
        found = jnp.where(slot_row == 2 * goal + b, returned[:, 64 * b:64 * b + 1], -2.0)
        row_best = jnp.maximum(row_best, jnp.max(found, axis=0, keepdims=True))
    best_ref[...] = row_best
    for copy in (*waits(*there), *waits(*back)):
        copy.wait_send()


def finish(best_ref, mean_ref, row_ref, keep_ref, cluster_ref):
    best = best_ref[0]
    row_ref[...] = best
    keep_ref[...] = (best < cutoff).astype(jnp.int32)
    cluster_ref[...] = mean_ref[0, : cluster_ref.shape[0]]


def body(embeddings, cluster_id, member_order, cluster_slot, cluster_size):
    rows, width = embeddings.shape
    clusters = cluster_slot.shape[0]
    slots = clusters
    vmem = pl.BlockSpec(memory_space=pltpu.VMEM)
    best, mean = pl.pallas_call(
        kernel,
        out_shape=(
            jax.ShapeDtypeStruct((1, rows), jnp.float32),
            jax.ShapeDtypeStruct((1, 128), jnp.float32),
        ),
        in_specs=[pl.BlockSpec(memory_space=pltpu.HBM)] * 5,
        out_specs=(vmem, vmem),
        scratch_shapes=[
            pltpu.VMEM((1, rows), jnp.int32),
            pltpu.VMEM((1, rows), jnp.int32),
            pltpu.VMEM((1, clusters), jnp.int32),
            pltpu.VMEM((1, clusters), jnp.int32),
            pltpu.VMEM((rows, width), jnp.float32),
            pltpu.VMEM((rows, width), jnp.bfloat16),
            pltpu.VMEM((slots, width + TAG), jnp.bfloat16),
            pltpu.VMEM((slots, width + TAG), jnp.bfloat16),
            pltpu.VMEM((slots, 128), jnp.float32),
            pltpu.VMEM((N, 128), jnp.float32),
            pltpu.VMEM((N, 128), jnp.float32),
            pltpu.SemaphoreType.DMA((8,)),
            pltpu.SemaphoreType.DMA,
            pltpu.SemaphoreType.DMA((SEMS,)),
            pltpu.SemaphoreType.DMA((SEMS,)),
            pltpu.SemaphoreType.DMA((SEMS,)),
            pltpu.SemaphoreType.DMA((SEMS,)),
        ],
        compiler_params=pltpu.CompilerParams(collective_id=0, has_side_effects=True, vmem_limit_bytes=67_043_328),
    )(embeddings, cluster_id[None], member_order[None], cluster_slot[None], cluster_size[None])
    return pl.pallas_call(
        finish,
        out_shape=(
            jax.ShapeDtypeStruct((rows,), jnp.float32),
            jax.ShapeDtypeStruct((rows,), jnp.int32),
            jax.ShapeDtypeStruct((clusters // N,), jnp.float32),
        ),
        in_specs=[vmem, vmem],
        out_specs=(vmem, vmem, vmem),
    )(best, mean)


def solution(mesh):
    placed = (P(("rep", "dev"), None), P(("rep", "dev")), P(("rep", "dev")), P("rep"), P("rep"))
    return jax.shard_map(
        body,
        mesh=mesh,
        in_specs=placed,
        out_specs=(P(("rep", "dev")), P(("rep", "dev")), P(("rep", "dev"))),
        check_vma=False,
    )
```

```python
import functools

import jax
import jax.numpy as jnp
from jax import lax
from jax.experimental import pallas as pl
from jax.experimental.pallas import tpu as pltpu
from jax.sharding import PartitionSpec as P

norm_eps = 1e-06
cutoff = 0.8
MESH = pl.DeviceIdType.MESH
NY, NX, NZ = 4, 4, 8
N = NY * NX * NZ
OFFSETS = [(i // (NX * NZ), i // NZ % NX, i % NZ) for i in range(N)]
TAG = 128


def shifted(me, dy, dx, dz):
    y, x, z = me // (NX * NZ), me // NZ % NX, me % NZ
    return (y + dy) % NY * (NX * NZ) + (x + dx) % NX * NZ + (z + dz) % NZ


def peer(me, i):
    return shifted(me, *OFFSETS[i])


def source(me, i):
    dy, dx, dz = OFFSETS[i]
    return shifted(me, NY - dy, NX - dx, NZ - dz)


ORDER = [
    i
    for dy in (2, 3, 1, 0)
    for dx in (2, 1, 3, 0)
    for dz in (4, 3, 5, 2, 6, 1, 7, 0)
    for i in [(dy * NX + dx) * NZ + dz]
    if i
]
SEMS = N // NZ + NZ


def flag(i):
    return i // NZ if i >= NZ else N // NZ + i


def exchange(src, dst, send_sem, recv_sem, target, unit):
    for i in ORDER:
        pair = pl.ds(unit * i, unit)
        pltpu.make_async_remote_copy(
            src.at[pair], dst.at[pair], send_sem.at[flag(i)], recv_sem.at[flag(i)],
            device_id={"dev": target(i)}, device_id_type=MESH,
        ).start()


def waits(src, dst, send_sem, recv_sem, target, unit, groups=range(N // NZ)):
    for g in groups:
        if g == 0:
            continue
        part = pl.ds(unit * NZ * g, unit * NZ)
        yield pltpu.make_async_remote_copy(
            src.at[part], dst.at[part], send_sem.at[g], recv_sem.at[g],
            device_id={"dev": target(1)}, device_id_type=MESH,
        )
    for i in range(1, NZ) if 0 in groups else ():
        pair = pl.ds(unit * i, unit)
        yield pltpu.make_async_remote_copy(
            src.at[pair], dst.at[pair], send_sem.at[flag(i)], recv_sem.at[flag(i)],
            device_id={"dev": target(1)}, device_id_type=MESH,
        )


def kernel(emb_ref, id_hbm, order_hbm, slot_hbm, size_hbm, best_ref, mean_ref,
           id_ref, order_ref, slot_ref, size_ref, raw, unit, packed, got, spread, answers, returned, load_sem, own_sem, send_sem, recv_sem, back_send, back_recv):
    me = lax.axis_index("dev")
    rows, width = raw.shape
    slots = packed.shape[0]
    pieces = 4
    step = rows // pieces
    smalls = []
    for p, (src, dst) in enumerate(
        ((id_hbm, id_ref), (slot_hbm, slot_ref), (order_hbm, order_ref), (size_hbm, size_ref))
    ):
        load = pltpu.make_async_copy(src, dst, load_sem.at[pieces + p])
        load.start()
        smalls.append(load)
    loads = []
    for p in range(pieces):
        part = pl.ds(p * step, step)
        load = pltpu.make_async_copy(emb_ref.at[part], raw.at[part], load_sem.at[p])
        load.start()
        loads.append(load)
    barrier = pltpu.get_barrier_semaphore()
    for i in ORDER:
        pl.semaphore_signal(barrier, inc=1, device_id={"dev": peer(me, i)}, device_id_type=MESH)

    for load in smalls:
        load.wait()
    member = lax.broadcasted_iota(jnp.int32, (slots, rows), 0) == id_ref[...]
    table = jnp.broadcast_to(slot_ref[...].astype(jnp.bfloat16), (8, slots))
    slot_row = jnp.dot(table, member.astype(jnp.bfloat16), preferred_element_type=jnp.float32)[0:1]
    slot_row = slot_row.astype(jnp.int32)
    place = lax.broadcasted_iota(jnp.int32, (slots, rows), 0)
    offset = place // 2
    goal = shifted(me, offset // (NX * NZ), offset // NZ % NX, offset % NZ)
    chosen = slot_row == goal * 2 + place % 2
    pick = chosen.astype(jnp.bfloat16)
    rank_next = (order_ref[...] + 1).astype(jnp.float32)
    tag = jnp.sum(jnp.where(chosen, rank_next, 0.0), axis=1, keepdims=True)
    packed[:, width:] = jnp.broadcast_to(tag, (slots, TAG)).astype(jnp.bfloat16)

    for p in range(pieces):
        loads[p].wait()
        part = pl.ds(p * step, step)
        values = raw[part]
        squares_sum = jnp.sum(values * values, axis=1, keepdims=True)
        unit[part] = (values * lax.rsqrt(squares_sum + norm_eps)).astype(jnp.bfloat16)
    chunk = 512
    for k in range(0, width, chunk):
        packed[:, k:k + chunk] = jnp.dot(
            pick, unit[:, k:k + chunk], preferred_element_type=jnp.float32
        ).astype(jnp.bfloat16)

    pl.semaphore_wait(barrier, N - 1)
    there = (packed, got, send_sem, recv_sem, functools.partial(peer, me), 2)
    exchange(*there)
    own = pltpu.make_async_copy(packed.at[pl.ds(0, 2)], got.at[pl.ds(0, 2)], own_sem)
    own.start()
    own.wait()
    sizes = [
        jnp.sum(jnp.where(slot_ref[...] == 2 * me + b, size_ref[...], 0), axis=1, keepdims=True).astype(jnp.float32)
        for b in range(2)
    ]
    first = (lax.broadcasted_iota(jnp.int32, (8, TAG), 1) == 0).astype(jnp.bfloat16)

    def arrive(groups):
        for copy in waits(*there, groups):
            copy.wait_recv()

    def gram(start, count, start_j, count_j):
        total = jnp.zeros((count, count_j), jnp.float32)
        chunk = 1024
        for k in range(0, width, chunk):
            total += lax.dot_general(
                got[start:start + count, k:k + chunk], got[start_j:start_j + count_j, k:k + chunk],
                (((1,), (1,)), ((), ())), preferred_element_type=jnp.float32,
            )
        return total

    def rows_of(start, count):
        rank = got[start:start + count, width:][:, 0:1].astype(jnp.float32)
        side = lax.broadcasted_iota(jnp.int32, (count, 1), 0) % 2
        live = (rank > 0.0) & (rank <= jnp.where(side == 0, sizes[0], sizes[1]))
        return jnp.where(live, rank, -1.0), side

    def columns_of(start, count):
        rank = lax.dot_general(
            first, got[start:start + count, width:], (((1,), (1,)), ((), ())), preferred_element_type=jnp.float32
        )[0:1]
        side = lax.broadcasted_iota(jnp.int32, (1, count), 1) % 2
        live = (rank > 0.0) & (rank <= jnp.where(side == 0, sizes[0], sizes[1]))
        return jnp.where(live, rank, 1024.0), side

    def nearest(similar, row, column):
        allowed = (row[1] == column[1]) & (column[0] < row[0])
        return jnp.max(jnp.where(allowed, similar, -1.0), axis=1, keepdims=True)

    low, mid, high = (0, slots // 4), (slots // 4, slots // 4), (slots // 2, slots // 2)
    arrive(range(8, 16))
    row_c, column_c = rows_of(*high), columns_of(*high)
    best_c = nearest(gram(*high, *high), row_c, column_c)
    arrive(range(4, 8))
    row_b, column_b = rows_of(*mid), columns_of(*mid)
    best_b = nearest(gram(*mid, *mid), row_b, column_b)
    across = gram(*mid, *high)
    best_b = jnp.maximum(best_b, nearest(across, row_b, column_c))
    best_c = jnp.maximum(best_c, nearest(across.T, row_c, column_b))
    arrive(range(4))
    row_a, column_a = rows_of(*low), columns_of(*low)
    last = gram(*low, 0, slots)
    best_a = jnp.maximum(
        nearest(last[:, :slots // 2], row_a, columns_of(0, slots // 2)),
        nearest(last[:, slots // 2:], row_a, column_c),
    )
    turned = last.T
    best_b = jnp.maximum(best_b, nearest(turned[slots // 4:slots // 2], row_b, column_a))
    best_c = jnp.maximum(best_c, nearest(turned[slots // 2:], row_c, column_a))
    best = jnp.concatenate([best_a, best_b, best_c], axis=0)
    rank_i = jnp.concatenate([row_a[0], row_b[0], row_c[0]], axis=0)
    live_i = rank_i > 0.0
    side_i = lax.broadcasted_iota(jnp.int32, (slots, 1), 0) % 2
    spread[...] = jnp.broadcast_to(best, spread.shape)
    halves = [spread[pl.ds(b, N, stride=2), :] for b in range(2)]
    lane = lax.broadcasted_iota(jnp.int32, (1, 128), 1)
    answers[...] = jnp.where(lane < 64, halves[0], halves[1])

    back = (answers, returned, back_send, back_recv, functools.partial(source, me), 1)
    exchange(*back)
    own = pltpu.make_async_copy(answers.at[pl.ds(0, 1)], returned.at[pl.ds(0, 1)], own_sem)
    own.start()
    means = [
        jnp.sum(jnp.where(live_i & (side_i == b), best, 0.0), axis=0, keepdims=True) / sizes[b]
        for b in range(2)
    ]
    mean_ref[...] = jnp.where(lane == 0, means[0], means[1])
    own.wait()
    for copy in waits(*back):
        copy.wait_recv()
    offset = lax.broadcasted_iota(jnp.int32, (N, rows), 0)
    goal = shifted(me, offset // (NX * NZ), offset // NZ % NX, offset % NZ)
    row_best = jnp.full((1, rows), -2.0, jnp.float32)
    for b in range(2):
        found = jnp.where(slot_row == 2 * goal + b, returned[:, 64 * b:64 * b + 1], -2.0)
        row_best = jnp.maximum(row_best, jnp.max(found, axis=0, keepdims=True))
    best_ref[...] = row_best
    for copy in (*waits(*there), *waits(*back)):
        copy.wait_send()


def finish(best_ref, mean_ref, row_ref, keep_ref, cluster_ref):
    best = best_ref[0]
    row_ref[...] = best
    keep_ref[...] = (best < cutoff).astype(jnp.int32)
    cluster_ref[...] = mean_ref[0, : cluster_ref.shape[0]]


def body(embeddings, cluster_id, member_order, cluster_slot, cluster_size):
    rows, width = embeddings.shape
    clusters = cluster_slot.shape[0]
    slots = clusters
    vmem = pl.BlockSpec(memory_space=pltpu.VMEM)
    best, mean = pl.pallas_call(
        kernel,
        out_shape=(pltpu.VMEM((1, rows), jnp.float32), pltpu.VMEM((1, 128), jnp.float32)),
        in_specs=[pl.BlockSpec(memory_space=pltpu.HBM)] * 5,
        out_specs=(vmem, vmem),
        scratch_shapes=[
            pltpu.VMEM((1, rows), jnp.int32),
            pltpu.VMEM((1, rows), jnp.int32),
            pltpu.VMEM((1, clusters), jnp.int32),
            pltpu.VMEM((1, clusters), jnp.int32),
            pltpu.VMEM((rows, width), jnp.float32),
            pltpu.VMEM((rows, width), jnp.bfloat16),
            pltpu.VMEM((slots, width + TAG), jnp.bfloat16),
            pltpu.VMEM((slots, width + TAG), jnp.bfloat16),
            pltpu.VMEM((slots, 128), jnp.float32),
            pltpu.VMEM((N, 128), jnp.float32),
            pltpu.VMEM((N, 128), jnp.float32),
            pltpu.SemaphoreType.DMA((8,)),
            pltpu.SemaphoreType.DMA,
            pltpu.SemaphoreType.DMA((SEMS,)),
            pltpu.SemaphoreType.DMA((SEMS,)),
            pltpu.SemaphoreType.DMA((SEMS,)),
            pltpu.SemaphoreType.DMA((SEMS,)),
        ],
        compiler_params=pltpu.CompilerParams(collective_id=0, has_side_effects=True, vmem_limit_bytes=32 * 1024 * 1024),
    )(*(
        pltpu.with_memory_space_constraint(x, pltpu.HBM)
        for x in (embeddings, cluster_id[None], member_order[None], cluster_slot[None], cluster_size[None])
    ))
    return pl.pallas_call(
        finish,
        out_shape=(
            jax.ShapeDtypeStruct((rows,), jnp.float32),
            jax.ShapeDtypeStruct((rows,), jnp.int32),
            jax.ShapeDtypeStruct((clusters // N,), jnp.float32),
        ),
        in_specs=[vmem, vmem],
        out_specs=(vmem, vmem, vmem),
        compiler_params=pltpu.CompilerParams(vmem_limit_bytes=1024 * 1024),
    )(pltpu.with_memory_space_constraint(best, pltpu.VMEM), pltpu.with_memory_space_constraint(mean, pltpu.VMEM))


def solution(mesh):
    placed = (P(("rep", "dev"), None), P(("rep", "dev")), P(("rep", "dev")), P("rep"), P("rep"))
    return jax.shard_map(
        body,
        mesh=mesh,
        in_specs=placed,
        out_specs=(P(("rep", "dev")), P(("rep", "dev")), P(("rep", "dev"))),
        check_vma=False,
    )
```

```python
import functools

import jax
import jax.numpy as jnp
from jax import lax
from jax.experimental import pallas as pl
from jax.experimental.pallas import tpu as pltpu
from jax.sharding import PartitionSpec as P

norm_eps = 1e-06
cutoff = 0.8
MESH = pl.DeviceIdType.MESH
NY, NX, NZ = 4, 4, 8
N = NY * NX * NZ
OFFSETS = [(i // (NX * NZ), i // NZ % NX, i % NZ) for i in range(N)]


def shifted(me, dy, dx, dz):
    y, x, z = me // (NX * NZ), me // NZ % NX, me % NZ
    return (y + dy) % NY * (NX * NZ) + (x + dx) % NX * NZ + (z + dz) % NZ


def peer(me, i):
    return shifted(me, *OFFSETS[i])


def source(me, i):
    dy, dx, dz = OFFSETS[i]
    return shifted(me, NY - dy, NX - dx, NZ - dz)


ORDER = [
    i
    for dy in (2, 3, 1, 0)
    for dx in (2, 1, 3, 0)
    for dz in (4, 3, 5, 2, 6, 1, 7, 0)
    for i in [(dy * NX + dx) * NZ + dz]
    if i
]
SEMS = N // NZ + NZ


def flag(i):
    return i // NZ if i >= NZ else N // NZ + i


def exchange(src, dst, send_sem, recv_sem, target, unit, order=ORDER):
    for i in order:
        pair = pl.ds(unit * i, unit)
        pltpu.make_async_remote_copy(
            src.at[pair], dst.at[pair], send_sem.at[flag(i)], recv_sem.at[flag(i)],
            device_id={"dev": target(i)}, device_id_type=MESH,
        ).start()


def waits(src, dst, send_sem, recv_sem, target, unit, groups=range(N // NZ)):
    for g in groups:
        if g == 0:
            continue
        part = pl.ds(unit * NZ * g, unit * NZ)
        yield pltpu.make_async_remote_copy(
            src.at[part], dst.at[part], send_sem.at[g], recv_sem.at[g],
            device_id={"dev": target(1)}, device_id_type=MESH,
        )
    for i in range(1, NZ) if 0 in groups else ():
        pair = pl.ds(unit * i, unit)
        yield pltpu.make_async_remote_copy(
            src.at[pair], dst.at[pair], send_sem.at[flag(i)], recv_sem.at[flag(i)],
            device_id={"dev": target(1)}, device_id_type=MESH,
        )


def kernel(emb_ref, id_hbm, order_hbm, slot_hbm, size_hbm, best_ref, mean_ref,
           id_ref, order_ref, slot_ref, size_ref, raw, unit, packed, got, ranks, spoken, column, heard, spread, answers, returned, load_sem, own_sem, send_sem, recv_sem,
           back_send, back_recv, speak_send, speak_recv, pass_send, pass_recv):
    me = lax.axis_index("dev")
    rows, width = raw.shape
    slots = packed.shape[0]
    pieces = 4
    step = rows // pieces
    smalls = []
    for p, (src, dst) in enumerate(
        ((id_hbm, id_ref), (slot_hbm, slot_ref), (order_hbm, order_ref), (size_hbm, size_ref))
    ):
        load = pltpu.make_async_copy(src, dst, load_sem.at[pieces + p])
        load.start()
        smalls.append(load)
    loads = []
    for p in range(pieces):
        part = pl.ds(p * step, step)
        load = pltpu.make_async_copy(emb_ref.at[part], raw.at[part], load_sem.at[p])
        load.start()
        loads.append(load)
    barrier = pltpu.get_barrier_semaphore()
    for i in ORDER:
        pl.semaphore_signal(barrier, inc=1, device_id={"dev": peer(me, i)}, device_id_type=MESH)

    for load in smalls:
        load.wait()
    member = lax.broadcasted_iota(jnp.int32, (slots, rows), 0) == id_ref[...]
    table = jnp.broadcast_to(slot_ref[...].astype(jnp.bfloat16), (8, slots))
    slot_row = jnp.dot(table, member.astype(jnp.bfloat16), preferred_element_type=jnp.float32)[0:1]
    slot_row = slot_row.astype(jnp.int32)
    place = lax.broadcasted_iota(jnp.int32, (slots, rows), 0)
    offset = place // 2
    goal = shifted(me, offset // (NX * NZ), offset // NZ % NX, offset % NZ)
    chosen = slot_row == goal * 2 + place % 2
    pick = chosen.astype(jnp.bfloat16)
    rank_next = (order_ref[...] + 1).astype(jnp.float32)
    said = lax.dot_general(
        jnp.broadcast_to(rank_next, (8, rows)).astype(jnp.bfloat16), pick, (((1,), (1,)), ((), ())),
        preferred_element_type=jnp.float32,
    )
    slot_lane = lax.broadcasted_iota(jnp.int32, (NZ, slots), 1)
    said = jnp.where(slot_lane // 2 % NZ == lax.broadcasted_iota(jnp.int32, (NZ, slots), 0), said, 0.0)
    slot_line = lax.broadcasted_iota(jnp.int32, (slots, 128), 0)
    fold = lax.broadcasted_iota(jnp.int32, (slots, 128), 1) == slot_line // (2 * NZ) * 2 + slot_line % 2
    said = jnp.dot(said.astype(jnp.bfloat16), fold.astype(jnp.bfloat16), preferred_element_type=jnp.float32)
    spoken[...] = said
    column[0:1] = said[0:1]

    for p in range(pieces):
        loads[p].wait()
        part = pl.ds(p * step, step)
        values = raw[part]
        squares_sum = jnp.sum(values * values, axis=1, keepdims=True)
        unit[part] = (values * lax.rsqrt(squares_sum + norm_eps)).astype(jnp.bfloat16)
    chunk = 512
    for k in range(0, width, chunk):
        packed[:, k:k + chunk] = jnp.dot(
            pick, unit[:, k:k + chunk], preferred_element_type=jnp.float32
        ).astype(jnp.bfloat16)

    pl.semaphore_wait(barrier, N - 1)
    there = (packed, got, send_sem, recv_sem, functools.partial(peer, me), 2)
    speak = [
        pltpu.make_async_remote_copy(
            spoken.at[pl.ds(dz, 1)], column.at[pl.ds(dz, 1)], speak_send.at[dz], speak_recv.at[dz],
            device_id={"dev": shifted(me, 0, 0, dz)}, device_id_type=MESH,
        )
        for dz in range(1, NZ)
    ]
    for copy in speak:
        copy.start()
    early = len(ORDER) // 4
    exchange(*there, ORDER[:early])
    for copy in speak:
        copy.wait_recv()
    forward = [
        pltpu.make_async_remote_copy(
            column, heard.at[q], pass_send.at[q], pass_recv.at[q],
            device_id={"dev": shifted(me, q // NX, q % NX, 0)}, device_id_type=MESH,
        )
        for q in range(1, NY * NX)
    ]
    for copy in forward:
        copy.start()
    exchange(*there, ORDER[early:])
    own = pltpu.make_async_copy(packed.at[pl.ds(0, 2)], got.at[pl.ds(0, 2)], own_sem)
    own.start()
    own.wait()
    sizes = [
        jnp.sum(jnp.where(slot_ref[...] == 2 * me + b, size_ref[...], 0), axis=1, keepdims=True).astype(jnp.float32)
        for b in range(2)
    ]
    heard[0] = column[...]
    for copy in forward:
        copy.wait_recv()
    told = heard[...].reshape(N, 128)
    told_line = lax.broadcasted_iota(jnp.int32, (N, 128), 0) // NZ * 2
    told_lane = lax.broadcasted_iota(jnp.int32, (N, 128), 1)
    for b in range(2):
        rank = jnp.sum(jnp.where(told_lane == told_line + b, told, 0.0), axis=1, keepdims=True)
        ranks[pl.ds(b, N, stride=2), :] = jnp.broadcast_to(rank, (N, 128))

    def arrive(groups):
        for copy in waits(*there, groups):
            copy.wait_recv()

    def gram(start, count, start_j, count_j):
        total = jnp.zeros((count, count_j), jnp.float32)
        chunk = 1024
        for k in range(0, width, chunk):
            total += lax.dot_general(
                got[start:start + count, k:k + chunk], got[start_j:start_j + count_j, k:k + chunk],
                (((1,), (1,)), ((), ())), preferred_element_type=jnp.float32,
            )
        return total

    def rows_of(start, count):
        rank = ranks[start:start + count, 0:1]
        side = lax.broadcasted_iota(jnp.int32, (count, 1), 0) % 2
        live = (rank > 0.0) & (rank <= jnp.where(side == 0, sizes[0], sizes[1]))
        return jnp.where(live, rank, -1.0), side

    def columns_of(start, count):
        rank = ranks[start:start + count, :].T[0:1]
        side = lax.broadcasted_iota(jnp.int32, (1, count), 1) % 2
        live = (rank > 0.0) & (rank <= jnp.where(side == 0, sizes[0], sizes[1]))
        return jnp.where(live, rank, 1024.0), side

    def nearest(similar, row, column):
        allowed = (row[1] == column[1]) & (column[0] < row[0])
        return jnp.max(jnp.where(allowed, similar, -1.0), axis=1, keepdims=True)

    low, mid, high = (0, slots // 4), (slots // 4, slots // 4), (slots // 2, slots // 2)
    row_a, column_a = rows_of(*low), columns_of(*low)
    row_b, column_b = rows_of(*mid), columns_of(*mid)
    row_c, column_c = rows_of(*high), columns_of(*high)
    column_ab = columns_of(0, slots // 2)
    arrive(range(8, 16))
    best_c = nearest(gram(*high, *high), row_c, column_c)
    arrive(range(4, 8))
    best_b = nearest(gram(*mid, *mid), row_b, column_b)
    across = gram(*mid, *high)
    best_b = jnp.maximum(best_b, nearest(across, row_b, column_c))
    best_c = jnp.maximum(best_c, nearest(across.T, row_c, column_b))
    arrive(range(4))
    last = gram(*low, 0, slots)
    best_a = jnp.maximum(
        nearest(last[:, :slots // 2], row_a, column_ab),
        nearest(last[:, slots // 2:], row_a, column_c),
    )
    turned = last.T
    best_b = jnp.maximum(best_b, nearest(turned[slots // 4:slots // 2], row_b, column_a))
    best_c = jnp.maximum(best_c, nearest(turned[slots // 2:], row_c, column_a))
    best = jnp.concatenate([best_a, best_b, best_c], axis=0)
    rank_i = jnp.concatenate([row_a[0], row_b[0], row_c[0]], axis=0)
    live_i = rank_i > 0.0
    side_i = lax.broadcasted_iota(jnp.int32, (slots, 1), 0) % 2
    spread[...] = jnp.broadcast_to(best, spread.shape)
    halves = [spread[pl.ds(b, N, stride=2), :] for b in range(2)]
    lane = lax.broadcasted_iota(jnp.int32, (1, 128), 1)
    answers[...] = jnp.where(lane < 64, halves[0], halves[1])

    back = (answers, returned, back_send, back_recv, functools.partial(source, me), 1)
    exchange(*back)
    own = pltpu.make_async_copy(answers.at[pl.ds(0, 1)], returned.at[pl.ds(0, 1)], own_sem)
    own.start()
    means = [
        jnp.sum(jnp.where(live_i & (side_i == b), best, 0.0), axis=0, keepdims=True) / sizes[b]
        for b in range(2)
    ]
    mean_ref[...] = jnp.where(lane == 0, means[0], means[1])
    own.wait()
    for copy in waits(*back):
        copy.wait_recv()
    offset = lax.broadcasted_iota(jnp.int32, (N, rows), 0)
    goal = shifted(me, offset // (NX * NZ), offset // NZ % NX, offset % NZ)
    row_best = jnp.full((1, rows), -2.0, jnp.float32)
    for b in range(2):
        found = jnp.where(slot_row == 2 * goal + b, returned[:, 64 * b:64 * b + 1], -2.0)
        row_best = jnp.maximum(row_best, jnp.max(found, axis=0, keepdims=True))
    best_ref[...] = row_best
    for copy in (*waits(*there), *waits(*back), *speak, *forward):
        copy.wait_send()


def finish(best_ref, mean_ref, row_ref, keep_ref, cluster_ref):
    best = best_ref[0]
    row_ref[...] = best
    keep_ref[...] = (best < cutoff).astype(jnp.int32)
    cluster_ref[...] = mean_ref[0, : cluster_ref.shape[0]]


def body(embeddings, cluster_id, member_order, cluster_slot, cluster_size):
    rows, width = embeddings.shape
    clusters = cluster_slot.shape[0]
    slots = clusters
    vmem = pl.BlockSpec(memory_space=pltpu.VMEM)
    best, mean = pl.pallas_call(
        kernel,
        out_shape=(pltpu.VMEM((1, rows), jnp.float32), pltpu.VMEM((1, 128), jnp.float32)),
        in_specs=[pl.BlockSpec(memory_space=pltpu.HBM)] * 5,
        out_specs=(vmem, vmem),
        scratch_shapes=[
            pltpu.VMEM((1, rows), jnp.int32),
            pltpu.VMEM((1, rows), jnp.int32),
            pltpu.VMEM((1, clusters), jnp.int32),
            pltpu.VMEM((1, clusters), jnp.int32),
            pltpu.VMEM((rows, width), jnp.float32),
            pltpu.VMEM((rows, width), jnp.bfloat16),
            pltpu.VMEM((slots, width), jnp.bfloat16),
            pltpu.VMEM((slots, width), jnp.bfloat16),
            pltpu.VMEM((slots, 128), jnp.float32),
            pltpu.VMEM((NZ, 128), jnp.float32),
            pltpu.VMEM((NZ, 128), jnp.float32),
            pltpu.VMEM((NY * NX, NZ, 128), jnp.float32),
            pltpu.VMEM((slots, 128), jnp.float32),
            pltpu.VMEM((N, 128), jnp.float32),
            pltpu.VMEM((N, 128), jnp.float32),
            pltpu.SemaphoreType.DMA((8,)),
            pltpu.SemaphoreType.DMA,
            pltpu.SemaphoreType.DMA((SEMS,)),
            pltpu.SemaphoreType.DMA((SEMS,)),
            pltpu.SemaphoreType.DMA((SEMS,)),
            pltpu.SemaphoreType.DMA((SEMS,)),
            pltpu.SemaphoreType.DMA((NZ,)),
            pltpu.SemaphoreType.DMA((NZ,)),
            pltpu.SemaphoreType.DMA((NY * NX,)),
            pltpu.SemaphoreType.DMA((NY * NX,)),
        ],
        compiler_params=pltpu.CompilerParams(collective_id=0, has_side_effects=True, vmem_limit_bytes=32 * 1024 * 1024),
    )(*(
        pltpu.with_memory_space_constraint(x, pltpu.HBM)
        for x in (embeddings, cluster_id[None], member_order[None], cluster_slot[None], cluster_size[None])
    ))
    return pl.pallas_call(
        finish,
        out_shape=(
            jax.ShapeDtypeStruct((rows,), jnp.float32),
            jax.ShapeDtypeStruct((rows,), jnp.int32),
            jax.ShapeDtypeStruct((clusters // N,), jnp.float32),
        ),
        in_specs=[vmem, vmem],
        out_specs=(vmem, vmem, vmem),
        compiler_params=pltpu.CompilerParams(vmem_limit_bytes=1024 * 1024),
    )(pltpu.with_memory_space_constraint(best, pltpu.VMEM), pltpu.with_memory_space_constraint(mean, pltpu.VMEM))


def solution(mesh):
    placed = (P(("rep", "dev"), None), P(("rep", "dev")), P(("rep", "dev")), P("rep"), P("rep"))
    return jax.shard_map(
        body,
        mesh=mesh,
        in_specs=placed,
        out_specs=(P(("rep", "dev")), P(("rep", "dev")), P(("rep", "dev"))),
        check_vma=False,
    )
```

```python
import functools

import jax
import jax.numpy as jnp
from jax import lax
from jax.experimental import pallas as pl
from jax.experimental.pallas import tpu as pltpu
from jax.sharding import PartitionSpec as P

norm_eps = 1e-06
cutoff = 0.8
MESH = pl.DeviceIdType.MESH
NY, NX, NZ = 4, 4, 8
N = NY * NX * NZ
OFFSETS = [(i // (NX * NZ), i // NZ % NX, i % NZ) for i in range(N)]


def shifted(me, dy, dx, dz):
    y, x, z = me // (NX * NZ), me // NZ % NX, me % NZ
    return (y + dy) % NY * (NX * NZ) + (x + dx) % NX * NZ + (z + dz) % NZ


def peer(me, i):
    return shifted(me, *OFFSETS[i])


def source(me, i):
    dy, dx, dz = OFFSETS[i]
    return shifted(me, NY - dy, NX - dx, NZ - dz)


ORDER = [
    i
    for dy in (2, 3, 1, 0)
    for dx in (2, 1, 3, 0)
    for dz in (4, 3, 5, 2, 6, 1, 7, 0)
    for i in [(dy * NX + dx) * NZ + dz]
    if i
]


def hops(i):
    return sum(min(d, n - d) for d, n in zip(OFFSETS[i], (NY, NX, NZ)))


FAR_FIRST = sorted(ORDER, key=lambda i: -hops(i))
SEMS = N // NZ + NZ


def flag(i):
    return i // NZ if i >= NZ else N // NZ + i


def exchange(src, dst, send_sem, recv_sem, target, unit, order=ORDER):
    for i in order:
        pair = pl.ds(unit * i, unit)
        pltpu.make_async_remote_copy(
            src.at[pair], dst.at[pair], send_sem.at[flag(i)], recv_sem.at[flag(i)],
            device_id={"dev": target(i)}, device_id_type=MESH,
        ).start()


def waits(src, dst, send_sem, recv_sem, target, unit, groups=range(N // NZ)):
    for g in groups:
        if g == 0:
            continue
        part = pl.ds(unit * NZ * g, unit * NZ)
        yield pltpu.make_async_remote_copy(
            src.at[part], dst.at[part], send_sem.at[g], recv_sem.at[g],
            device_id={"dev": target(1)}, device_id_type=MESH,
        )
    for i in range(1, NZ) if 0 in groups else ():
        pair = pl.ds(unit * i, unit)
        yield pltpu.make_async_remote_copy(
            src.at[pair], dst.at[pair], send_sem.at[flag(i)], recv_sem.at[flag(i)],
            device_id={"dev": target(1)}, device_id_type=MESH,
        )


def kernel(emb_ref, id_hbm, order_hbm, slot_hbm, size_hbm, best_ref, mean_ref,
           id_ref, order_ref, slot_ref, size_ref, raw, unit, packed, got, ranks, spoken, column, heard, spread, answers, returned, load_sem, own_sem, send_sem, recv_sem,
           back_send, back_recv, speak_send, speak_recv, pass_send, pass_recv):
    me = lax.axis_index("dev")
    rows, width = raw.shape
    slots = packed.shape[0]
    barrier = pltpu.get_barrier_semaphore()
    for i in FAR_FIRST:
        pl.semaphore_signal(barrier, inc=1, device_id={"dev": peer(me, i)}, device_id_type=MESH)
    pieces = 4
    step = rows // pieces
    smalls = []
    for p, (src, dst) in enumerate(
        ((id_hbm, id_ref), (slot_hbm, slot_ref), (order_hbm, order_ref), (size_hbm, size_ref))
    ):
        load = pltpu.make_async_copy(src, dst, load_sem.at[pieces + p])
        load.start()
        smalls.append(load)
    loads = []
    for p in range(pieces):
        part = pl.ds(p * step, step)
        load = pltpu.make_async_copy(emb_ref.at[part], raw.at[part], load_sem.at[p])
        load.start()
        loads.append(load)

    for load in smalls:
        load.wait()
    member = lax.broadcasted_iota(jnp.int32, (slots, rows), 0) == id_ref[...]
    table = jnp.broadcast_to(slot_ref[...].astype(jnp.bfloat16), (8, slots))
    slot_row = jnp.dot(table, member.astype(jnp.bfloat16), preferred_element_type=jnp.float32)[0:1]
    slot_row = slot_row.astype(jnp.int32)
    place = lax.broadcasted_iota(jnp.int32, (slots, rows), 0)
    offset = place // 2
    goal = shifted(me, offset // (NX * NZ), offset // NZ % NX, offset % NZ)
    chosen = slot_row == goal * 2 + place % 2
    pick = chosen.astype(jnp.bfloat16)
    rank_next = (order_ref[...] + 1).astype(jnp.float32)
    said = lax.dot_general(
        jnp.broadcast_to(rank_next, (8, rows)).astype(jnp.bfloat16), pick, (((1,), (1,)), ((), ())),
        preferred_element_type=jnp.float32,
    )
    slot_lane = lax.broadcasted_iota(jnp.int32, (NZ, slots), 1)
    said = jnp.where(slot_lane // 2 % NZ == lax.broadcasted_iota(jnp.int32, (NZ, slots), 0), said, 0.0)
    slot_line = lax.broadcasted_iota(jnp.int32, (slots, 128), 0)
    fold = lax.broadcasted_iota(jnp.int32, (slots, 128), 1) == slot_line // (2 * NZ) * 2 + slot_line % 2
    said = jnp.dot(said.astype(jnp.bfloat16), fold.astype(jnp.bfloat16), preferred_element_type=jnp.float32)
    spoken[...] = said
    column[0:1] = said[0:1]

    for p in range(pieces):
        loads[p].wait()
        part = pl.ds(p * step, step)
        values = raw[part]
        squares_sum = jnp.sum(values * values, axis=1, keepdims=True)
        unit[part] = (values * lax.rsqrt(squares_sum + norm_eps)).astype(jnp.bfloat16)
    chunk = 512
    for k in range(0, width, chunk):
        packed[:, k:k + chunk] = jnp.dot(
            pick, unit[:, k:k + chunk], preferred_element_type=jnp.float32
        ).astype(jnp.bfloat16)

    pl.semaphore_wait(barrier, N - 1)
    there = (packed, got, send_sem, recv_sem, functools.partial(peer, me), 2)
    speak = [
        pltpu.make_async_remote_copy(
            spoken.at[pl.ds(dz, 1)], column.at[pl.ds(dz, 1)], speak_send.at[dz], speak_recv.at[dz],
            device_id={"dev": shifted(me, 0, 0, dz)}, device_id_type=MESH,
        )
        for dz in range(1, NZ)
    ]
    for copy in speak:
        copy.start()
    early = len(ORDER) // 4
    exchange(*there, ORDER[:early])
    for copy in speak:
        copy.wait_recv()
    forward = [
        pltpu.make_async_remote_copy(
            column, heard.at[q], pass_send.at[q], pass_recv.at[q],
            device_id={"dev": shifted(me, q // NX, q % NX, 0)}, device_id_type=MESH,
        )
        for q in range(1, NY * NX)
    ]
    for copy in forward:
        copy.start()
    exchange(*there, ORDER[early:])
    own = pltpu.make_async_copy(packed.at[pl.ds(0, 2)], got.at[pl.ds(0, 2)], own_sem)
    own.start()
    own.wait()
    sizes = [
        jnp.sum(jnp.where(slot_ref[...] == 2 * me + b, size_ref[...], 0), axis=1, keepdims=True).astype(jnp.float32)
        for b in range(2)
    ]
    heard[0] = column[...]
    for copy in forward:
        copy.wait_recv()
    told = heard[...].reshape(N, 128)
    told_line = lax.broadcasted_iota(jnp.int32, (N, 128), 0) // NZ * 2
    told_lane = lax.broadcasted_iota(jnp.int32, (N, 128), 1)
    for b in range(2):
        rank = jnp.sum(jnp.where(told_lane == told_line + b, told, 0.0), axis=1, keepdims=True)
        ranks[pl.ds(b, N, stride=2), :] = jnp.broadcast_to(rank, (N, 128))

    def arrive(groups):
        for copy in waits(*there, groups):
            copy.wait_recv()

    def gram(start, count, start_j, count_j):
        total = jnp.zeros((count, count_j), jnp.float32)
        chunk = 1024
        for k in range(0, width, chunk):
            total += lax.dot_general(
                got[start:start + count, k:k + chunk], got[start_j:start_j + count_j, k:k + chunk],
                (((1,), (1,)), ((), ())), preferred_element_type=jnp.float32,
            )
        return total

    def rows_of(start, count):
        rank = ranks[start:start + count, 0:1]
        side = lax.broadcasted_iota(jnp.int32, (count, 1), 0) % 2
        live = (rank > 0.0) & (rank <= jnp.where(side == 0, sizes[0], sizes[1]))
        return jnp.where(live, rank, -1.0), side

    def columns_of(start, count):
        rank = ranks[start:start + count, :].T[0:1]
        side = lax.broadcasted_iota(jnp.int32, (1, count), 1) % 2
        live = (rank > 0.0) & (rank <= jnp.where(side == 0, sizes[0], sizes[1]))
        return jnp.where(live, rank, 1024.0), side

    def nearest(similar, row, column):
        allowed = (row[1] == column[1]) & (column[0] < row[0])
        return jnp.max(jnp.where(allowed, similar, -1.0), axis=1, keepdims=True)

    low, mid, high = (0, slots // 4), (slots // 4, slots // 4), (slots // 2, slots // 2)
    row_a, column_a = rows_of(*low), columns_of(*low)
    row_b, column_b = rows_of(*mid), columns_of(*mid)
    row_c, column_c = rows_of(*high), columns_of(*high)
    column_ab = columns_of(0, slots // 2)
    arrive(range(8, 16))
    best_c = nearest(gram(*high, *high), row_c, column_c)
    arrive(range(4, 8))
    best_b = nearest(gram(*mid, *mid), row_b, column_b)
    across = gram(*mid, *high)
    best_b = jnp.maximum(best_b, nearest(across, row_b, column_c))
    best_c = jnp.maximum(best_c, nearest(across.T, row_c, column_b))
    arrive(range(4))
    last = gram(*low, 0, slots)
    best_a = jnp.maximum(
        nearest(last[:, :slots // 2], row_a, column_ab),
        nearest(last[:, slots // 2:], row_a, column_c),
    )
    turned = last.T
    best_b = jnp.maximum(best_b, nearest(turned[slots // 4:slots // 2], row_b, column_a))
    best_c = jnp.maximum(best_c, nearest(turned[slots // 2:], row_c, column_a))
    best = jnp.concatenate([best_a, best_b, best_c], axis=0)
    rank_i = jnp.concatenate([row_a[0], row_b[0], row_c[0]], axis=0)
    live_i = rank_i > 0.0
    side_i = lax.broadcasted_iota(jnp.int32, (slots, 1), 0) % 2
    spread[...] = jnp.broadcast_to(best, spread.shape)
    halves = [spread[pl.ds(b, N, stride=2), :] for b in range(2)]
    lane = lax.broadcasted_iota(jnp.int32, (1, 128), 1)
    answers[...] = jnp.where(lane < 64, halves[0], halves[1])

    back = (answers, returned, back_send, back_recv, functools.partial(source, me), 1)
    exchange(*back, FAR_FIRST)
    own = pltpu.make_async_copy(answers.at[pl.ds(0, 1)], returned.at[pl.ds(0, 1)], own_sem)
    own.start()
    means = [
        jnp.sum(jnp.where(live_i & (side_i == b), best, 0.0), axis=0, keepdims=True) / sizes[b]
        for b in range(2)
    ]
    mean_ref[...] = jnp.where(lane == 0, means[0], means[1])
    offset = lax.broadcasted_iota(jnp.int32, (N, rows), 0)
    goal = shifted(me, offset // (NX * NZ), offset // NZ % NX, offset % NZ)
    mine = [slot_row == 2 * goal + b for b in range(2)]
    own.wait()
    for copy in waits(*back):
        copy.wait_recv()
    row_best = jnp.full((1, rows), -2.0, jnp.float32)
    for b in range(2):
        found = jnp.where(mine[b], returned[:, 64 * b:64 * b + 1], -2.0)
        row_best = jnp.maximum(row_best, jnp.max(found, axis=0, keepdims=True))
    best_ref[...] = row_best
    for copy in (*waits(*there), *waits(*back), *speak, *forward):
        copy.wait_send()


def finish(best_ref, mean_ref, row_ref, keep_ref, cluster_ref):
    best = best_ref[0]
    row_ref[...] = best
    keep_ref[...] = (best < cutoff).astype(jnp.int32)
    cluster_ref[...] = mean_ref[0, : cluster_ref.shape[0]]


def body(embeddings, cluster_id, member_order, cluster_slot, cluster_size):
    rows, width = embeddings.shape
    clusters = cluster_slot.shape[0]
    slots = clusters
    vmem = pl.BlockSpec(memory_space=pltpu.VMEM)
    best, mean = pl.pallas_call(
        kernel,
        out_shape=(pltpu.VMEM((1, rows), jnp.float32), pltpu.VMEM((1, 128), jnp.float32)),
        in_specs=[pl.BlockSpec(memory_space=pltpu.HBM)] * 5,
        out_specs=(vmem, vmem),
        scratch_shapes=[
            pltpu.VMEM((1, rows), jnp.int32),
            pltpu.VMEM((1, rows), jnp.int32),
            pltpu.VMEM((1, clusters), jnp.int32),
            pltpu.VMEM((1, clusters), jnp.int32),
            pltpu.VMEM((rows, width), jnp.float32),
            pltpu.VMEM((rows, width), jnp.bfloat16),
            pltpu.VMEM((slots, width), jnp.bfloat16),
            pltpu.VMEM((slots, width), jnp.bfloat16),
            pltpu.VMEM((slots, 128), jnp.float32),
            pltpu.VMEM((NZ, 128), jnp.float32),
            pltpu.VMEM((NZ, 128), jnp.float32),
            pltpu.VMEM((NY * NX, NZ, 128), jnp.float32),
            pltpu.VMEM((slots, 128), jnp.float32),
            pltpu.VMEM((N, 128), jnp.float32),
            pltpu.VMEM((N, 128), jnp.float32),
            pltpu.SemaphoreType.DMA((8,)),
            pltpu.SemaphoreType.DMA,
            pltpu.SemaphoreType.DMA((SEMS,)),
            pltpu.SemaphoreType.DMA((SEMS,)),
            pltpu.SemaphoreType.DMA((SEMS,)),
            pltpu.SemaphoreType.DMA((SEMS,)),
            pltpu.SemaphoreType.DMA((NZ,)),
            pltpu.SemaphoreType.DMA((NZ,)),
            pltpu.SemaphoreType.DMA((NY * NX,)),
            pltpu.SemaphoreType.DMA((NY * NX,)),
        ],
        compiler_params=pltpu.CompilerParams(collective_id=0, has_side_effects=True, vmem_limit_bytes=32 * 1024 * 1024),
    )(*(
        pltpu.with_memory_space_constraint(x, pltpu.HBM)
        for x in (embeddings, cluster_id[None], member_order[None], cluster_slot[None], cluster_size[None])
    ))
    return pl.pallas_call(
        finish,
        out_shape=(
            jax.ShapeDtypeStruct((rows,), jnp.float32),
            jax.ShapeDtypeStruct((rows,), jnp.int32),
            jax.ShapeDtypeStruct((clusters // N,), jnp.float32),
        ),
        in_specs=[vmem, vmem],
        out_specs=(vmem, vmem, vmem),
        compiler_params=pltpu.CompilerParams(vmem_limit_bytes=1024 * 1024),
    )(pltpu.with_memory_space_constraint(best, pltpu.VMEM), pltpu.with_memory_space_constraint(mean, pltpu.VMEM))


def solution(mesh):
    placed = (P(("rep", "dev"), None), P(("rep", "dev")), P(("rep", "dev")), P("rep"), P("rep"))
    return jax.shard_map(
        body,
        mesh=mesh,
        in_specs=placed,
        out_specs=(P(("rep", "dev")), P(("rep", "dev")), P(("rep", "dev"))),
        check_vma=False,
    )
```

```python
import functools

import jax
import jax.numpy as jnp
from jax import lax
from jax.experimental import pallas as pl
from jax.experimental.pallas import tpu as pltpu
from jax.sharding import PartitionSpec as P

norm_eps = 1e-06
cutoff = 0.8
MESH = pl.DeviceIdType.MESH
NY, NX, NZ = 4, 4, 8
N = NY * NX * NZ
OFFSETS = [(i // (NX * NZ), i // NZ % NX, i % NZ) for i in range(N)]


def shifted(me, dy, dx, dz):
    y, x, z = me // (NX * NZ), me // NZ % NX, me % NZ
    return (y + dy) % NY * (NX * NZ) + (x + dx) % NX * NZ + (z + dz) % NZ


def peer(me, i):
    return shifted(me, *OFFSETS[i])


def source(me, i):
    dy, dx, dz = OFFSETS[i]
    return shifted(me, NY - dy, NX - dx, NZ - dz)


ORDER = [
    i
    for dys in ((2, 3), (1,), (0,))
    for dx in (2, 1, 3, 0)
    for dy in dys
    for dz in (4, 3, 5, 2, 6, 1, 7, 0)
    for i in [(dy * NX + dx) * NZ + dz]
    if i
]


def hops(i):
    return sum(min(d, n - d) for d, n in zip(OFFSETS[i], (NY, NX, NZ)))


FAR_FIRST = sorted(ORDER, key=lambda i: -hops(i))
SEMS = N // NZ + NZ


def flag(i):
    return i // NZ if i >= NZ else N // NZ + i


def exchange(src, dst, send_sem, recv_sem, target, unit, order=ORDER):
    for i in order:
        pair = pl.ds(unit * i, unit)
        pltpu.make_async_remote_copy(
            src.at[pair], dst.at[pair], send_sem.at[flag(i)], recv_sem.at[flag(i)],
            device_id={"dev": target(i)}, device_id_type=MESH,
        ).start()


def waits(src, dst, send_sem, recv_sem, target, unit, groups=range(N // NZ)):
    for g in groups:
        if g == 0:
            continue
        part = pl.ds(unit * NZ * g, unit * NZ)
        yield pltpu.make_async_remote_copy(
            src.at[part], dst.at[part], send_sem.at[g], recv_sem.at[g],
            device_id={"dev": target(1)}, device_id_type=MESH,
        )
    for i in range(1, NZ) if 0 in groups else ():
        pair = pl.ds(unit * i, unit)
        yield pltpu.make_async_remote_copy(
            src.at[pair], dst.at[pair], send_sem.at[flag(i)], recv_sem.at[flag(i)],
            device_id={"dev": target(1)}, device_id_type=MESH,
        )


def kernel(emb_ref, id_hbm, order_hbm, slot_hbm, size_hbm, best_ref, mean_ref,
           id_ref, order_ref, slot_ref, size_ref, raw, unit, packed, got, ranks, spoken, column, heard, spread, answers, returned, load_sem, own_sem, send_sem, recv_sem,
           back_send, back_recv, speak_send, speak_recv, pass_send, pass_recv):
    me = lax.axis_index("dev")
    rows, width = raw.shape
    slots = packed.shape[0]
    barrier = pltpu.get_barrier_semaphore()
    for i in FAR_FIRST:
        pl.semaphore_signal(barrier, inc=1, device_id={"dev": peer(me, i)}, device_id_type=MESH)
    pieces = 4
    step = rows // pieces
    smalls = []
    for p, (src, dst) in enumerate(
        ((id_hbm, id_ref), (slot_hbm, slot_ref), (order_hbm, order_ref), (size_hbm, size_ref))
    ):
        load = pltpu.make_async_copy(src, dst, load_sem.at[pieces + p])
        load.start()
        smalls.append(load)
    loads = []
    for p in range(pieces):
        part = pl.ds(p * step, step)
        load = pltpu.make_async_copy(emb_ref.at[part], raw.at[part], load_sem.at[p])
        load.start()
        loads.append(load)

    for load in smalls:
        load.wait()
    member = lax.broadcasted_iota(jnp.int32, (slots, rows), 0) == id_ref[...]
    table = jnp.broadcast_to(slot_ref[...].astype(jnp.bfloat16), (8, slots))
    slot_row = jnp.dot(table, member.astype(jnp.bfloat16), preferred_element_type=jnp.float32)[0:1]
    slot_row = slot_row.astype(jnp.int32)
    place = lax.broadcasted_iota(jnp.int32, (slots, rows), 0)
    offset = place // 2
    goal = shifted(me, offset // (NX * NZ), offset // NZ % NX, offset % NZ)
    chosen = slot_row == goal * 2 + place % 2
    pick = chosen.astype(jnp.bfloat16)
    rank_next = (order_ref[...] + 1).astype(jnp.float32)
    said = lax.dot_general(
        jnp.broadcast_to(rank_next, (8, rows)).astype(jnp.bfloat16), pick, (((1,), (1,)), ((), ())),
        preferred_element_type=jnp.float32,
    )
    slot_lane = lax.broadcasted_iota(jnp.int32, (NZ, slots), 1)
    said = jnp.where(slot_lane // 2 % NZ == lax.broadcasted_iota(jnp.int32, (NZ, slots), 0), said, 0.0)
    slot_line = lax.broadcasted_iota(jnp.int32, (slots, 128), 0)
    fold = lax.broadcasted_iota(jnp.int32, (slots, 128), 1) == slot_line // (2 * NZ) * 2 + slot_line % 2
    said = jnp.dot(said.astype(jnp.bfloat16), fold.astype(jnp.bfloat16), preferred_element_type=jnp.float32)
    spoken[...] = said
    column[0:1] = said[0:1]

    for p in range(pieces):
        loads[p].wait()
        part = pl.ds(p * step, step)
        values = raw[part]
        squares_sum = jnp.sum(values * values, axis=1, keepdims=True)
        unit[part] = (values * lax.rsqrt(squares_sum + norm_eps)).astype(jnp.bfloat16)
    chunk = 512
    for k in range(0, width, chunk):
        packed[:, k:k + chunk] = jnp.dot(
            pick, unit[:, k:k + chunk], preferred_element_type=jnp.float32
        ).astype(jnp.bfloat16)

    pl.semaphore_wait(barrier, N - 1)
    there = (packed, got, send_sem, recv_sem, functools.partial(peer, me), 2)
    speak = [
        pltpu.make_async_remote_copy(
            spoken.at[pl.ds(dz, 1)], column.at[pl.ds(dz, 1)], speak_send.at[dz], speak_recv.at[dz],
            device_id={"dev": shifted(me, 0, 0, dz)}, device_id_type=MESH,
        )
        for dz in range(1, NZ)
    ]
    for copy in speak:
        copy.start()
    early = len(ORDER) // 4
    exchange(*there, ORDER[:early])
    for copy in speak:
        copy.wait_recv()
    forward = [
        pltpu.make_async_remote_copy(
            column, heard.at[q], pass_send.at[q], pass_recv.at[q],
            device_id={"dev": shifted(me, q // NX, q % NX, 0)}, device_id_type=MESH,
        )
        for q in range(1, NY * NX)
    ]
    for copy in forward:
        copy.start()
    exchange(*there, ORDER[early:])
    own = pltpu.make_async_copy(packed.at[pl.ds(0, 2)], got.at[pl.ds(0, 2)], own_sem)
    own.start()
    own.wait()
    sizes = [
        jnp.sum(jnp.where(slot_ref[...] == 2 * me + b, size_ref[...], 0), axis=1, keepdims=True).astype(jnp.float32)
        for b in range(2)
    ]
    heard[0] = column[...]
    for copy in forward:
        copy.wait_recv()
    told = heard[...].reshape(N, 128)
    told_line = lax.broadcasted_iota(jnp.int32, (N, 128), 0) // NZ * 2
    told_lane = lax.broadcasted_iota(jnp.int32, (N, 128), 1)
    for b in range(2):
        rank = jnp.sum(jnp.where(told_lane == told_line + b, told, 0.0), axis=1, keepdims=True)
        ranks[pl.ds(b, N, stride=2), :] = jnp.broadcast_to(rank, (N, 128))

    def arrive(groups):
        for copy in waits(*there, groups):
            copy.wait_recv()

    def gram(start, count, start_j, count_j):
        return lax.dot_general(
            got[start:start + count, :], got[start_j:start_j + count_j, :],
            (((1,), (1,)), ((), ())), preferred_element_type=jnp.float32,
        )

    def rows_of(start, count):
        rank = ranks[start:start + count, 0:1]
        side = lax.broadcasted_iota(jnp.int32, (count, 1), 0) % 2
        live = (rank > 0.0) & (rank <= jnp.where(side == 0, sizes[0], sizes[1]))
        return jnp.where(live, rank, -1.0), side

    def columns_of(start, count):
        rank = ranks[start:start + count, :].T[0:1]
        side = lax.broadcasted_iota(jnp.int32, (1, count), 1) % 2
        live = (rank > 0.0) & (rank <= jnp.where(side == 0, sizes[0], sizes[1]))
        return jnp.where(live, rank, 1024.0), side

    def nearest(similar, row, column):
        allowed = (row[1] == column[1]) & (column[0] < row[0])
        return jnp.max(jnp.where(allowed, similar, -1.0), axis=1, keepdims=True)

    low, mid, high = (0, slots // 4), (slots // 4, slots // 4), (slots // 2, slots // 2)
    row_a, column_a = rows_of(*low), columns_of(*low)
    row_b, column_b = rows_of(*mid), columns_of(*mid)
    row_c, column_c = rows_of(*high), columns_of(*high)
    column_ab = columns_of(0, slots // 2)
    arrive(range(8, 16))
    best_c = nearest(gram(*high, *high), row_c, column_c)
    arrive(range(4, 8))
    best_b = nearest(gram(*mid, *mid), row_b, column_b)
    across = gram(*mid, *high)
    best_b = jnp.maximum(best_b, nearest(across, row_b, column_c))
    best_c = jnp.maximum(best_c, nearest(across.T, row_c, column_b))
    arrive(range(4))
    last = gram(*low, 0, slots)
    best_a = jnp.maximum(
        nearest(last[:, :slots // 2], row_a, column_ab),
        nearest(last[:, slots // 2:], row_a, column_c),
    )
    turned = last.T
    best_b = jnp.maximum(best_b, nearest(turned[slots // 4:slots // 2], row_b, column_a))
    best_c = jnp.maximum(best_c, nearest(turned[slots // 2:], row_c, column_a))
    best = jnp.concatenate([best_a, best_b, best_c], axis=0)
    rank_i = jnp.concatenate([row_a[0], row_b[0], row_c[0]], axis=0)
    live_i = rank_i > 0.0
    side_i = lax.broadcasted_iota(jnp.int32, (slots, 1), 0) % 2
    spread[...] = jnp.broadcast_to(best, spread.shape)
    halves = [spread[pl.ds(b, N, stride=2), :] for b in range(2)]
    lane = lax.broadcasted_iota(jnp.int32, (1, 128), 1)
    answers[...] = jnp.where(lane < 64, halves[0], halves[1])

    back = (answers, returned, back_send, back_recv, functools.partial(source, me), 1)
    exchange(*back, FAR_FIRST)
    own = pltpu.make_async_copy(answers.at[pl.ds(0, 1)], returned.at[pl.ds(0, 1)], own_sem)
    own.start()
    means = [
        jnp.sum(jnp.where(live_i & (side_i == b), best, 0.0), axis=0, keepdims=True) / sizes[b]
        for b in range(2)
    ]
    mean_ref[...] = jnp.where(lane == 0, means[0], means[1])
    offset = lax.broadcasted_iota(jnp.int32, (N, rows), 0)
    goal = shifted(me, offset // (NX * NZ), offset // NZ % NX, offset % NZ)
    mine = [slot_row == 2 * goal + b for b in range(2)]
    own.wait()
    for copy in waits(*back):
        copy.wait_recv()
    row_best = jnp.full((1, rows), -2.0, jnp.float32)
    for b in range(2):
        found = jnp.where(mine[b], returned[:, 64 * b:64 * b + 1], -2.0)
        row_best = jnp.maximum(row_best, jnp.max(found, axis=0, keepdims=True))
    best_ref[...] = row_best
    for copy in (*waits(*there), *waits(*back), *speak, *forward):
        copy.wait_send()


def finish(best_ref, mean_ref, row_ref, keep_ref, cluster_ref):
    best = best_ref[0]
    row_ref[...] = best
    keep_ref[...] = (best < cutoff).astype(jnp.int32)
    cluster_ref[...] = mean_ref[0, : cluster_ref.shape[0]]


def body(embeddings, cluster_id, member_order, cluster_slot, cluster_size):
    rows, width = embeddings.shape
    clusters = cluster_slot.shape[0]
    slots = clusters
    vmem = pl.BlockSpec(memory_space=pltpu.VMEM)
    best, mean = pl.pallas_call(
        kernel,
        out_shape=(pltpu.VMEM((1, rows), jnp.float32), pltpu.VMEM((1, 128), jnp.float32)),
        in_specs=[pl.BlockSpec(memory_space=pltpu.HBM)] * 5,
        out_specs=(vmem, vmem),
        scratch_shapes=[
            pltpu.VMEM((1, rows), jnp.int32),
            pltpu.VMEM((1, rows), jnp.int32),
            pltpu.VMEM((1, clusters), jnp.int32),
            pltpu.VMEM((1, clusters), jnp.int32),
            pltpu.VMEM((rows, width), jnp.float32),
            pltpu.VMEM((rows, width), jnp.bfloat16),
            pltpu.VMEM((slots, width), jnp.bfloat16),
            pltpu.VMEM((slots, width), jnp.bfloat16),
            pltpu.VMEM((slots, 128), jnp.float32),
            pltpu.VMEM((NZ, 128), jnp.float32),
            pltpu.VMEM((NZ, 128), jnp.float32),
            pltpu.VMEM((NY * NX, NZ, 128), jnp.float32),
            pltpu.VMEM((slots, 128), jnp.float32),
            pltpu.VMEM((N, 128), jnp.float32),
            pltpu.VMEM((N, 128), jnp.float32),
            pltpu.SemaphoreType.DMA((8,)),
            pltpu.SemaphoreType.DMA,
            pltpu.SemaphoreType.DMA((SEMS,)),
            pltpu.SemaphoreType.DMA((SEMS,)),
            pltpu.SemaphoreType.DMA((SEMS,)),
            pltpu.SemaphoreType.DMA((SEMS,)),
            pltpu.SemaphoreType.DMA((NZ,)),
            pltpu.SemaphoreType.DMA((NZ,)),
            pltpu.SemaphoreType.DMA((NY * NX,)),
            pltpu.SemaphoreType.DMA((NY * NX,)),
        ],
        compiler_params=pltpu.CompilerParams(collective_id=0, has_side_effects=True, vmem_limit_bytes=32 * 1024 * 1024),
    )(*(
        pltpu.with_memory_space_constraint(x, pltpu.HBM)
        for x in (embeddings, cluster_id[None], member_order[None], cluster_slot[None], cluster_size[None])
    ))
    return pl.pallas_call(
        finish,
        out_shape=(
            jax.ShapeDtypeStruct((rows,), jnp.float32),
            jax.ShapeDtypeStruct((rows,), jnp.int32),
            jax.ShapeDtypeStruct((clusters // N,), jnp.float32),
        ),
        in_specs=[vmem, vmem],
        out_specs=(vmem, vmem, vmem),
        compiler_params=pltpu.CompilerParams(vmem_limit_bytes=1024 * 1024),
    )(pltpu.with_memory_space_constraint(best, pltpu.VMEM), pltpu.with_memory_space_constraint(mean, pltpu.VMEM))


def solution(mesh):
    placed = (P(("rep", "dev"), None), P(("rep", "dev")), P(("rep", "dev")), P("rep"), P("rep"))
    return jax.shard_map(
        body,
        mesh=mesh,
        in_specs=placed,
        out_specs=(P(("rep", "dev")), P(("rep", "dev")), P(("rep", "dev"))),
        check_vma=False,
    )
```
